512 devices in a mesh: head: 8 (over z_hi, core), vis: 64 (over y, x, z_lo).
Axes of the slice: x: 4, y: 8, z: 8 (z_hi: 4, z_lo: 2; z = z_hi * 2 + z_lo), core: 2. Of those that a mesh axis runs over, the one named last changes fastest.
Arguments:
- queries: bfloat16 [2, 512, 4096], P(None, 'vis', 'head'), may hold values from -24 to 24
- keys: bfloat16 [2, 25600, 1024], P(None, 'vis', 'head'), may hold values from -24 to 24
- values: bfloat16 [2, 25600, 1024], P(None, 'vis', 'head'), may hold values from -6 to 6
- d_out: bfloat16 [2, 512, 4096], P(None, 'vis', 'head'), may hold values from -6 to 6
- q_weight: bfloat16 [4096, 4096], P('vis', 'head'), may hold values from -0.09375 to 0.09375
Outputs:
- d_input: bfloat16 [2, 512, 4096], P(None, 'head', 'vis')
- d_keys: bfloat16 [2, 25600, 1024], P(None, 'vis', 'head')
- d_values: bfloat16 [2, 25600, 1024], P(None, 'vis', 'head')
The draws below stay inside these ranges and needn't reach their ends.
All inputs are finite; a program needn't handle non-finite values.
Results may differ from the reference program's by a relative error of at most 0.014.
Values may be sent and summed in bfloat16 or wider, within the bound.
No kernel may reach another device: no remote copies, remote signals or barrier semaphores. Data moves between devices by JAX's collectives and lax.ppermute only.
A program may use at most 64 MiB of HBM per device.

```python
import jax
import jax.numpy as jnp
from jax import lax

D = 4096
HQ = 32
KVH = 8
HD = 128
BATCH = 2
TEXT = 512
VIS = 25600


def draw_queries(key, part):
    width = HQ * HD
    drawn = jnp.clip(jax.random.normal(jax.random.fold_in(key, 11), (BATCH, TEXT, width), jnp.float32), -6.0, 6.0)
    return drawn.astype(jnp.bfloat16)


def draw_keys(key, part):
    width = KVH * HD
    drawn = jnp.clip(jax.random.normal(jax.random.fold_in(key, 23), (BATCH, VIS, width), jnp.float32), -6.0, 6.0)
    return drawn.astype(jnp.bfloat16)


def levels(stream_key, dims, pieces, smallest, largest):
    def one(dim, parts):
        heights = jax.random.uniform(jax.random.fold_in(jax.random.fold_in(stream_key, 6), dim), (parts,), jnp.float32, smallest / len(pieces), largest / len(pieces))
        return jnp.repeat(jnp.exp(heights), dims[dim] // parts).reshape((-1,) + (1,) * (len(dims) - dim - 1))

    gain = one(*pieces[0])
    for cut in pieces[1:]:
        gain = gain * one(*cut)
    return gain


def noise(stream_key, dims, deviation, bound, pieces=(), dtype=jnp.bfloat16):
    values = jax.random.normal(stream_key, dims, jnp.float32) * deviation
    if len(pieces) > 0:
        values = levels(stream_key, dims, pieces, -0.22, 0.18) * values
    return jnp.clip(values, min=-bound, max=bound).astype(dtype)


def setup_inputs(seed: int = 0) -> dict:
    seeds = jax.random.split(jax.random.key(seed), 6)
    queries = draw_queries(jax.random.fold_in(seeds[5], 71), 0)
    keys = draw_keys(jax.random.fold_in(seeds[5], 71), 0)
    values = noise(seeds[2], (BATCH, VIS, KVH * HD), 1.0, 6.0, ((1, 64), (2, 8)))
    d_out = noise(seeds[3], (BATCH, TEXT, HQ * HD), 1.0, 6.0, ((1, 64), (2, 8)))
    q_weight = noise(seeds[4], (D, HQ * HD), (HQ * HD) ** -0.5, 0.09375, ((0, 64), (1, 8)))
    return dict(queries=queries, keys=keys, values=values, d_out=d_out, q_weight=q_weight)


def group_backward(operands):
    query_group, grad_group, key_group, value_group = operands
    inv_root = HD ** -0.5
    query_full = query_group.astype(jnp.float32)
    grad_full = grad_group.astype(jnp.float32)
    key_full = key_group.astype(jnp.float32)
    value_full = value_group.astype(jnp.float32)
    scores = jnp.einsum("btgd,bjd->bgtj", query_full, key_full) * inv_root
    log_total = jax.nn.logsumexp(scores, axis=-1, keepdims=True)
    probs = jnp.exp(scores - log_total)
    probs_low = lax.optimization_barrier(probs.astype(jnp.bfloat16)).astype(jnp.float32)
    grad_probs = jnp.einsum("btgd,bjd->bgtj", grad_full, value_full)
    delta_sum = jnp.sum(probs * grad_probs, axis=-1, keepdims=True)
    grad_scores = probs * (grad_probs - delta_sum)
    grad_low = lax.optimization_barrier(grad_scores.astype(jnp.bfloat16)).astype(jnp.float32)
    grad_query = (jnp.einsum("bgtj,bjd->btgd", grad_low, key_full) * inv_root).astype(jnp.bfloat16)
    grad_key = (jnp.einsum("bgtj,btgd->bjd", grad_low, query_full) * inv_root).astype(jnp.bfloat16)
    grad_value = jnp.einsum("bgtj,btgd->bjd", probs_low, grad_full).astype(jnp.bfloat16)
    return grad_query, grad_key, grad_value


def reference(queries, keys, values, d_out, q_weight):
    groups = HQ // KVH
    batch_size, text_len, _ = queries.shape
    vis_len = keys.shape[1]
    query_heads = jnp.moveaxis(queries.reshape(batch_size, text_len, KVH, groups, HD), 2, 0)
    grad_heads = jnp.moveaxis(d_out.reshape(batch_size, text_len, KVH, groups, HD), 2, 0)
    key_heads = jnp.moveaxis(keys.reshape(batch_size, vis_len, KVH, HD), 2, 0)
    value_heads = jnp.moveaxis(values.reshape(batch_size, vis_len, KVH, HD), 2, 0)
    grad_query, grad_key, grad_value = lax.map(group_backward, (query_heads, grad_heads, key_heads, value_heads))
    grad_query = jnp.moveaxis(grad_query, 0, 2).reshape(batch_size, text_len, KVH * groups * HD)
    d_keys = jnp.moveaxis(grad_key, 0, 2).reshape(batch_size, vis_len, KVH * HD)
    d_values = jnp.moveaxis(grad_value, 0, 2).reshape(batch_size, vis_len, KVH * HD)
    d_input = jnp.einsum("btq,dq->btd", grad_query.astype(jnp.float32), q_weight.astype(jnp.float32))
    return d_input.astype(jnp.bfloat16), d_keys, d_values
```

```python
import jax
import jax.numpy as jnp
from jax import lax
from jax.sharding import Mesh
from jax.sharding import PartitionSpec as P

HQ = 32
KVH = 8
HD = 128
GROUPS = HQ // KVH
VIS = ("vis_0", "vis_1", "vis_2")
PAIR = "vis_2"
SCALE = HD ** (-0.5)
BF16 = jnp.bfloat16
F32 = jnp.float32


def exchanged(pieces, axes):
    return lax.all_to_all(pieces, axes, split_axis=0, concat_axis=0, tiled=True)


def swapped(array):
    return lax.ppermute(array, PAIR, [(0, 1), (1, 0)])


def rounded(array):
    return lax.reduce_precision(array, exponent_bits=8, mantissa_bits=7)


def in_pieces(array, count):
    out = []
    for _ in range(count):
        piece = rounded(array)
        out.append(piece.astype(BF16))
        array = array - piece
    return out


def whole_again(pieces):
    total = pieces[-1].astype(F32)
    for piece in reversed(pieces[:-1]):
        total = total + piece.astype(F32)
    return total


def first_pass(query, grad, keys, values):
    scores = jnp.einsum("jd,tgd->gjt", keys, query, preferred_element_type=F32) * SCALE
    peak = rounded(jnp.max(scores, axis=1))
    weights = jnp.exp(scores - peak[:, None])
    grad_probs = jnp.einsum("jd,tgd->gjt", values, grad, preferred_element_type=F32)
    total = jnp.sum(weights, axis=1)
    mean = jnp.sum(weights * grad_probs, axis=1) / total
    low = weights.astype(BF16)
    centred = (weights * (grad_probs - mean[:, None])).astype(BF16)
    term_a = jnp.einsum("gjt,jd->tgd", centred, keys, preferred_element_type=F32)
    term_b = jnp.einsum("gjt,jd->tgd", low, keys, preferred_element_type=F32)
    return peak, total, mean, low, centred, term_a.astype(BF16), term_b.astype(BF16)


def second_pass(low, centred, query, grad, scale, shift):
    by_row = scale.T[..., None]
    grad_scaled = (grad.astype(F32) * by_row).astype(BF16)
    query_scaled = (query.astype(F32) * by_row).astype(BF16)
    query_shifted = (query.astype(F32) * (by_row * shift.T[..., None])).astype(BF16)
    d_values = jnp.einsum("gjt,tgd->jd", low, grad_scaled, preferred_element_type=F32)
    d_keys = jnp.einsum("gjt,tgd->jd", centred, query_scaled, preferred_element_type=F32)
    d_keys = d_keys + jnp.einsum("gjt,tgd->jd", low, query_shifted, preferred_element_type=F32)
    return (d_keys * SCALE).astype(BF16), d_values.astype(BF16)


def per_device(queries, keys, values, d_out, q_weight):
    batch, rows, width = queries.shape
    shards = lax.axis_size(VIS)
    half = shards // batch
    heads = lax.axis_size("head")
    text = rows * shards
    lines = rows * GROUPS
    mine = lax.axis_index(PAIR)

    def pick(array, which):
        return jnp.where(which == 0, array[0], array[1])

    def in_order(own, other):
        return jnp.where(mine == 0, jnp.stack([own, other]), jnp.stack([other, own]))

    both = jnp.stack([keys, values])
    own_kv = jnp.where(mine == 0, both[:, 0], both[:, 1])
    other_kv = swapped(jnp.where(mine == 0, both[:, 1], both[:, 0]))
    kv = jnp.concatenate([own_kv, other_kv], axis=1)
    weight = in_order(q_weight, swapped(q_weight))

    sent = jnp.stack([queries, d_out], axis=1)
    sent = jnp.broadcast_to(sent, (half, *sent.shape)).reshape(shards, 2, rows, width)
    whole = exchanged(sent, VIS)
    query = whole[:, 0].reshape(text, GROUPS, HD)
    grad = whole[:, 1].reshape(text, GROUPS, HD)

    peak, total, mean, low, centred, term_a, term_b = first_pass(query, grad, kv[0], kv[1])

    def stat_lines(pieces):
        packed = jnp.stack([p.reshape(GROUPS, shards, rows) for p in pieces])
        packed = packed.transpose(2, 0, 3, 1).reshape(shards, -1)
        packed = jnp.pad(packed, ((0, 0), (0, -packed.shape[1] % HD)))
        return packed.reshape(shards, -1, HD)

    stats = stat_lines(in_pieces(peak, 1) + in_pieces(total, 2) + in_pieces(mean, 3))
    terms = [term_a.reshape(shards, lines, HD), term_b.reshape(shards, lines, HD), stats]
    home = exchanged(jnp.concatenate(terms, axis=1), VIS)
    home = home.reshape(half, batch, -1, HD)
    home_a = home[:, :, :lines].astype(F32)
    home_b = home[:, :, lines : 2 * lines].astype(F32)
    home_stats = home[:, :, 2 * lines :].reshape(half, batch, -1)[:, :, : 6 * lines]
    home_stats = home_stats.reshape(half, batch, 6, lines)
    peaks = home_stats[:, :, 0].astype(F32)
    totals = whole_again([home_stats[:, :, k] for k in (1, 2)])
    means = whole_again([home_stats[:, :, k] for k in (3, 4, 5)])
    peak_all = jnp.max(peaks, axis=0)
    share = jnp.exp(peaks - peak_all) * totals
    total_all = jnp.sum(share, axis=0)
    delta = jnp.sum(share * means, axis=0) / total_all
    factor = jnp.exp(peaks - peak_all) / total_all
    dq = jnp.sum(factor[..., None] * home_a + (factor * (means - delta))[..., None] * home_b, axis=0)
    dq_low = (dq * SCALE).astype(BF16)
    log_total = peak_all + jnp.log(total_all)

    back = jnp.stack(in_pieces(log_total, 3) + in_pieces(delta, 3), axis=1).reshape(batch, -1)
    back = jnp.pad(back, ((0, 0), (0, -back.shape[1] % HD))).reshape(batch, -1, HD)
    back = jnp.concatenate([dq_low, back], axis=1)
    back = jnp.broadcast_to(back, (half, *back.shape)).reshape(shards, -1, HD)
    spread = exchanged(back, VIS)
    dq_all = spread[:, :lines].reshape(heads, 2, text // heads // 2, width)
    row_stats = spread[:, lines:].reshape(shards, -1)[:, : 6 * lines].reshape(shards, 6, rows, GROUPS)
    row_stats = row_stats.transpose(1, 3, 0, 2).reshape(6, GROUPS, text)
    log_rows = whole_again([row_stats[k] for k in (0, 1, 2)])
    delta_rows = whole_again([row_stats[k] for k in (3, 4, 5)])

    part = jnp.einsum("hstq,zdq->hztsd", dq_all, weight, preferred_element_type=F32)
    part = part.astype(BF16).reshape(heads * 2, text // heads // 2, -1)
    arrived = exchanged(part, ("head", PAIR)).reshape(heads, batch, text // heads // 2, 2, -1)
    d_input = jnp.sum(arrived.astype(F32), axis=0).astype(BF16)
    d_input = d_input.transpose(0, 2, 1, 3).reshape(batch, text // heads, -1)

    d_keys, d_values = second_pass(
        low, centred, query, grad, jnp.exp(peak - log_rows), mean - delta_rows
    )
    d_kv = jnp.stack([d_keys, d_values])
    vis_rows = keys.shape[1]
    returned = swapped(d_kv[:, vis_rows:])
    d_kv = in_order(d_kv[:, :vis_rows], returned)
    return d_input, d_kv[:, 0], d_kv[:, 1]


def solution(mesh):
    torus = Mesh(
        mesh.devices.reshape(mesh.shape["head"], 8, 4, 2), ("head", "vis_0", "vis_1", "vis_2")
    )
    return jax.shard_map(
        per_device,
        mesh=torus,
        in_specs=(
            P(None, VIS, "head"),
            P(None, VIS, "head"),
            P(None, VIS, "head"),
            P(None, VIS, "head"),
            P(VIS, "head"),
        ),
        out_specs=(P(None, "head", VIS), P(None, VIS, "head"), P(None, VIS, "head")),
        check_vma=False,
    )
```

```python
import jax
import jax.numpy as jnp
from jax import lax
from jax.sharding import Mesh
from jax.sharding import PartitionSpec as P

HQ = 32
KVH = 8
HD = 128
GROUPS = HQ // KVH
ALONG = "vis_0"
GROUP = ("vis_1", "vis_2")
VIS = (ALONG, *GROUP)
SCALE = HD ** (-0.5)
BF16 = jnp.bfloat16
F32 = jnp.float32


def exchanged(pieces, axes):
    return lax.all_to_all(pieces, axes, split_axis=0, concat_axis=0, tiled=True)


def copies(array, count):
    return jnp.broadcast_to(array, (count, *array.shape))


def rounded(array):
    return lax.reduce_precision(array, exponent_bits=8, mantissa_bits=7)


def in_pieces(array, count):
    out = []
    for _ in range(count):
        piece = rounded(array)
        out.append(piece.astype(BF16))
        array = array - piece
    return out


def whole_again(pieces):
    total = pieces[-1].astype(F32)
    for piece in reversed(pieces[:-1]):
        total = total + piece.astype(F32)
    return total


def first_pass(query, grad, keys, values):
    scores = jnp.einsum("jd,td->jt", keys, query, preferred_element_type=F32) * SCALE
    peak = rounded(jnp.max(scores, axis=0))
    weights = jnp.exp(scores - peak)
    grad_probs = jnp.einsum("jd,td->jt", values, grad, preferred_element_type=F32)
    total = jnp.sum(weights, axis=0)
    mean = jnp.sum(weights * grad_probs, axis=0) / total
    low = weights.astype(BF16)
    centred = (weights * (grad_probs - mean)).astype(BF16)
    term_a = jnp.einsum("jt,jd->td", centred, keys, preferred_element_type=F32)
    term_b = jnp.einsum("jt,jd->td", low, keys, preferred_element_type=F32)
    terms = jnp.concatenate([term_a.astype(BF16), term_b.astype(BF16)], axis=1)
    return peak, total, mean, low, centred, terms


def second_pass(low, centred, query, grad, scale, shift):
    by_row = scale[:, None]
    grad_scaled = (grad.astype(F32) * by_row).astype(BF16)
    query_scaled = (query.astype(F32) * (by_row * SCALE)).astype(BF16)
    query_shifted = (query.astype(F32) * ((scale * shift)[:, None] * SCALE)).astype(BF16)
    d_values = jnp.einsum("jt,td->jd", low, grad_scaled, preferred_element_type=F32)
    d_keys = jnp.einsum("jt,td->jd", centred, query_scaled, preferred_element_type=F32)
    d_keys = d_keys + jnp.einsum("jt,td->jd", low, query_shifted, preferred_element_type=F32)
    return jnp.concatenate([d_keys.astype(BF16), d_values.astype(BF16)], axis=1)


def per_device(queries, keys, values, d_out, q_weight):
    batch, rows, width = queries.shape
    vis_rows = keys.shape[1]
    d_rows = q_weight.shape[0]
    heads = lax.axis_size("head")
    steps = lax.axis_size(ALONG)
    group = lax.axis_size(GROUP)
    text = rows * steps * group
    block = text // steps
    here = lax.axis_index(ALONG)

    def by_head(array):
        return array.reshape(batch, rows, GROUPS, HD).transpose(2, 0, 1, 3)

    sent = jnp.concatenate([by_head(queries), by_head(d_out)], axis=-1).reshape(group, rows, 2 * HD)
    sent = copies(sent, steps).reshape(steps * group, rows, 2 * HD)
    whole = exchanged(sent, VIS).reshape(text, 2 * HD)

    key_values = copies(jnp.concatenate([keys, values], axis=-1), GROUPS)
    key_values = key_values.reshape(group, vis_rows, 2 * HD)
    weight = q_weight.reshape(2, d_rows // 2, GROUPS, HD).transpose(2, 1, 0, 3)
    weight = jnp.repeat(weight.reshape(GROUPS, d_rows // 2, 2 * HD), batch, axis=0)
    near = exchanged(jnp.concatenate([key_values, weight], axis=1), GROUP)
    kv = near[:, :vis_rows].reshape(group * vis_rows, 2 * HD)
    weight = near[:, vis_rows:].reshape(group, d_rows // 2, 2, HD).transpose(0, 2, 1, 3)
    weight = weight.reshape(group, d_rows, HD)
    blank = jnp.zeros_like(weight)
    weight = jnp.concatenate(
        [jnp.concatenate([weight, blank], axis=2), jnp.concatenate([blank, weight], axis=2)], axis=1
    )

    query, grad = whole[:, :HD], whole[:, HD:]
    peak, total, mean, low, centred, terms = first_pass(query, grad, kv[:, :HD], kv[:, HD:])

    stats = jnp.stack(in_pieces(peak, 1) + in_pieces(total, 2) + in_pieces(mean, 3))
    stats = stats.reshape(-1, 2 * HD)
    parcel = [terms.reshape(steps, block, 2 * HD), copies(stats, steps)]
    home = exchanged(jnp.concatenate(parcel, axis=1), ALONG)
    home_terms = home[:, :block].astype(F32)
    home_stats = home[:, block:].reshape(steps, 6, text)
    peaks = home_stats[:, 0].astype(F32)
    totals = whole_again([home_stats[:, k] for k in (1, 2)])
    means = whole_again([home_stats[:, k] for k in (3, 4, 5)])
    peak_all = jnp.max(peaks, axis=0)
    factor = jnp.exp(peaks - peak_all)
    share = factor * totals
    total_all = jnp.sum(share, axis=0)
    delta = jnp.sum(share * means, axis=0) / total_all
    factor = factor / total_all
    shift = means - delta

    mine = lax.dynamic_slice_in_dim(jnp.stack([factor, factor * shift]), here * block, block, 2)
    dq = jnp.sum(
        mine[0][..., None] * home_terms[..., :HD] + mine[1][..., None] * home_terms[..., HD:], axis=0
    )
    dq_low = (dq * SCALE).astype(BF16).reshape(2, block // 2, HD).transpose(1, 0, 2)
    dq_low = dq_low.reshape(block // 2, 2 * HD)
    dq_all = exchanged(copies(dq_low, steps), ALONG)

    part = jnp.einsum("hrk,snk->hsrn", dq_all, weight, preferred_element_type=F32).astype(BF16)
    part = part.reshape(heads * group, block // 2, 2 * d_rows)
    arrived = exchanged(part, ("head", *GROUP))
    arrived = arrived.reshape(heads * GROUPS, batch, block // 2, 2, d_rows)
    d_input = jnp.sum(arrived.astype(F32), axis=0).astype(BF16)
    d_input = d_input.transpose(0, 2, 1, 3).reshape(batch, block, d_rows)

    scale = lax.dynamic_index_in_dim(factor, here, 0, keepdims=False)
    moved = lax.dynamic_index_in_dim(shift, here, 0, keepdims=False)
    d_kv = second_pass(low, centred, query, grad, scale, moved).reshape(group, vis_rows, 2 * HD)
    d_kv = exchanged(d_kv, GROUP).reshape(GROUPS, batch, vis_rows, 2 * HD)
    d_kv = jnp.sum(d_kv.astype(F32), axis=0).astype(BF16)
    return d_input, d_kv[..., :HD], d_kv[..., HD:]


def solution(mesh):
    torus = Mesh(
        mesh.devices.reshape(mesh.shape["head"], 8, 4, 2), ("head", "vis_0", "vis_1", "vis_2")
    )
    return jax.shard_map(
        per_device,
        mesh=torus,
        in_specs=(
            P(None, VIS, "head"),
            P(None, VIS, "head"),
            P(None, VIS, "head"),
            P(None, VIS, "head"),
            P(VIS, "head"),
        ),
        out_specs=(P(None, "head", VIS), P(None, VIS, "head"), P(None, VIS, "head")),
        check_vma=False,
    )
```

```python
import jax
import jax.numpy as jnp
from jax import lax
from jax.sharding import Mesh
from jax.sharding import PartitionSpec as P

HQ = 32
KVH = 8
HD = 128
GROUPS = HQ // KVH
ALONG = "vis_0"
ACROSS = "vis_1"
PAIR = "vis_2"
GROUP = (ACROSS, PAIR)
VIS = (ALONG, *GROUP)
SCALE = HD ** (-0.5)
BF16 = jnp.bfloat16
F32 = jnp.float32


def exchanged(pieces, axes):
    return lax.all_to_all(pieces, axes, split_axis=0, concat_axis=0, tiled=True)


def swapped(array, axis, distance):
    size = lax.axis_size(axis)
    return lax.ppermute(array, axis, [(k, k ^ distance) for k in range(size)])


def copies(array, count):
    return jnp.broadcast_to(array, (count, *array.shape))


def rounded(array):
    return lax.reduce_precision(array, exponent_bits=8, mantissa_bits=7)


def in_pieces(array, count):
    out = []
    for _ in range(count):
        piece = rounded(array)
        out.append(piece.astype(BF16))
        array = array - piece
    return out


def whole_again(pieces):
    total = pieces[-1].astype(F32)
    for piece in reversed(pieces[:-1]):
        total = total + piece.astype(F32)
    return total


def first_pass(query, grad, keys, values):
    scores = jnp.einsum("jd,td->jt", keys, query, preferred_element_type=F32) * SCALE
    peak = rounded(jnp.max(scores, axis=0))
    weights = jnp.exp(scores - peak)
    grad_probs = jnp.einsum("jd,td->jt", values, grad, preferred_element_type=F32)
    total = jnp.sum(weights, axis=0)
    mean = jnp.sum(weights * grad_probs, axis=0) / total
    low = weights.astype(BF16)
    centred = (weights * (grad_probs - mean)).astype(BF16)
    term_a = jnp.einsum("jt,jd->td", centred, keys, preferred_element_type=F32)
    term_b = jnp.einsum("jt,jd->td", low, keys, preferred_element_type=F32)
    terms = jnp.concatenate([term_a.astype(BF16), term_b.astype(BF16)], axis=1)
    return peak, total, mean, low, centred, terms


def second_pass(low, centred, query, grad, scale, shift):
    by_row = scale[:, None]
    grad_scaled = (grad.astype(F32) * by_row).astype(BF16)
    query_scaled = (query.astype(F32) * (by_row * SCALE)).astype(BF16)
    query_shifted = (query.astype(F32) * ((scale * shift)[:, None] * SCALE)).astype(BF16)
    d_values = jnp.einsum("jt,td->jd", low, grad_scaled, preferred_element_type=F32)
    d_keys = jnp.einsum("jt,td->jd", centred, query_scaled, preferred_element_type=F32)
    d_keys = d_keys + jnp.einsum("jt,td->jd", low, query_shifted, preferred_element_type=F32)
    return jnp.concatenate([d_keys.astype(BF16), d_values.astype(BF16)], axis=1)


def per_device(queries, keys, values, d_out, q_weight):
    batch, rows, width = queries.shape
    vis_rows = keys.shape[1]
    d_rows = q_weight.shape[0]
    heads = lax.axis_size("head")
    steps = lax.axis_size(ALONG)
    group = lax.axis_size(GROUP)
    text = rows * steps * group
    block = text // steps
    here = lax.axis_index(ALONG)

    def by_head(array):
        return array.reshape(batch, rows, GROUPS, HD).transpose(2, 0, 1, 3)

    sent = jnp.concatenate([by_head(queries), by_head(d_out)], axis=-1).reshape(group, rows, 2 * HD)
    sent = copies(sent, steps).reshape(steps * group, rows, 2 * HD)
    whole = exchanged(sent, VIS).reshape(text, 2 * HD)

    across = lax.axis_index(ACROSS)
    mine = lax.axis_index(PAIR)

    both = jnp.concatenate([keys, values], axis=-1)
    weight = q_weight.reshape(2, d_rows // 2, GROUPS, HD).transpose(2, 1, 0, 3)
    weight = weight.reshape(GROUPS * d_rows // 2, 2 * HD)
    own = jnp.where(mine == 0, both[0], both[1])
    other = jnp.where(mine == 0, both[1], both[0])
    other = swapped(jnp.concatenate([other, weight]), PAIR, 1)
    pair = jnp.stack([own, other[:vis_rows]])
    weight = jnp.where(
        mine == 0, jnp.stack([weight, other[vis_rows:]]), jnp.stack([other[vis_rows:], weight])
    )
    weight = weight.reshape(batch, GROUPS, d_rows // 2, 2 * HD)

    def weight_for(distance):
        return lax.dynamic_index_in_dim(weight, across ^ distance, 1, keepdims=False)

    near = [jnp.concatenate([pair, weight_for(k)], axis=1) for k in range(GROUPS)]
    near = jnp.stack([near[0]] + [swapped(near[k], ACROSS, k) for k in range(1, GROUPS)])
    kv = near[:, :, :vis_rows].reshape(group * vis_rows, 2 * HD)
    weight = near[:, :, vis_rows:].reshape(GROUPS, batch, d_rows // 2, 2, HD)
    weight = weight[jnp.arange(GROUPS) ^ across]
    weight = weight.transpose(0, 1, 3, 2, 4).reshape(group, d_rows, HD)
    blank = jnp.zeros_like(weight)
    weight = jnp.concatenate(
        [jnp.concatenate([weight, blank], axis=2), jnp.concatenate([blank, weight], axis=2)], axis=1
    )

    query, grad = whole[:, :HD], whole[:, HD:]
    peak, total, mean, low, centred, terms = first_pass(query, grad, kv[:, :HD], kv[:, HD:])

    stats = jnp.stack(in_pieces(peak, 1) + in_pieces(total, 2) + in_pieces(mean, 3))
    stats = stats.reshape(-1, 2 * HD)
    parcel = [terms.reshape(steps, block, 2 * HD), copies(stats, steps)]
    home = exchanged(jnp.concatenate(parcel, axis=1), ALONG)
    home_terms = home[:, :block].astype(F32)
    home_stats = home[:, block:].reshape(steps, 6, text)
    peaks = home_stats[:, 0].astype(F32)
    totals = whole_again([home_stats[:, k] for k in (1, 2)])
    means = whole_again([home_stats[:, k] for k in (3, 4, 5)])
    peak_all = jnp.max(peaks, axis=0)
    factor = jnp.exp(peaks - peak_all)
    share = factor * totals
    total_all = jnp.sum(share, axis=0)
    delta = jnp.sum(share * means, axis=0) / total_all
    factor = factor / total_all
    shift = means - delta

    local = lax.dynamic_slice_in_dim(jnp.stack([factor, factor * shift]), here * block, block, 2)
    dq = jnp.sum(
        local[0][..., None] * home_terms[..., :HD] + local[1][..., None] * home_terms[..., HD:], axis=0
    )
    dq_low = (dq * SCALE).astype(BF16).reshape(2, block // 2, HD).transpose(1, 0, 2)
    dq_low = dq_low.reshape(block // 2, 2 * HD)
    dq_all = exchanged(copies(dq_low, steps), ALONG)

    part = jnp.einsum("hrk,snk->hsrn", dq_all, weight, preferred_element_type=F32).astype(BF16)
    part = part.reshape(heads * group, block // 2, 2 * d_rows)
    arrived = exchanged(part, ("head", *GROUP))
    arrived = arrived.reshape(heads * GROUPS, batch, block // 2, 2, d_rows)
    d_input = jnp.sum(arrived.astype(F32), axis=0).astype(BF16)
    d_input = d_input.transpose(0, 2, 1, 3).reshape(batch, block, d_rows)

    scale = lax.dynamic_index_in_dim(factor, here, 0, keepdims=False)
    moved = lax.dynamic_index_in_dim(shift, here, 0, keepdims=False)
    d_kv = second_pass(low, centred, query, grad, scale, moved)
    d_kv = d_kv.reshape(GROUPS, batch, vis_rows, 2 * HD)
    total_kv = d_kv[0].astype(F32)
    for k in range(1, GROUPS):
        total_kv = total_kv + swapped(d_kv[k], ACROSS, k).astype(F32)
    total_kv = total_kv.astype(BF16)
    own, other = total_kv[0], swapped(total_kv[1], PAIR, 1)
    d_kv = jnp.where(mine == 0, jnp.stack([own, other]), jnp.stack([other, own]))
    return d_input, d_kv[..., :HD], d_kv[..., HD:]


def solution(mesh):
    torus = Mesh(
        mesh.devices.reshape(mesh.shape["head"], 8, 4, 2), ("head", "vis_0", "vis_1", "vis_2")
    )
    return jax.shard_map(
        per_device,
        mesh=torus,
        in_specs=(
            P(None, VIS, "head"),
            P(None, VIS, "head"),
            P(None, VIS, "head"),
            P(None, VIS, "head"),
            P(VIS, "head"),
        ),
        out_specs=(P(None, "head", VIS), P(None, VIS, "head"), P(None, VIS, "head")),
        check_vma=False,
    )
```
